32 devices in a mesh: dp: 8 (over z, x), rep: 4 (over y, core).
Axes of the slice: x: 2, y: 2, z: 4, core: 2. Of those that a mesh axis runs over, the one named last changes fastest.
Arguments:
- features: bfloat16 [5120, 8192], P('dp', 'rep'), may hold values from -6 to 6
- out_grads: bfloat16 [5120, 1024], P('dp'), may hold values from -12 to 12, as said below
- cold_sums: bfloat16 [8, 8192, 1024], P('dp', 'rep'), may hold values from -96 to 96
- weight: float32 [8192, 1024], P(('rep', 'dp')), may hold values from -3 to 3
- moment: float32 [8192, 1024], P(('rep', 'dp')), may hold values from -6 to 6
- second: float32 [8192, 1024], P(('rep', 'dp')), may hold values from 0.01 to 4
- ranks: int32 [8], replicated, may hold values from 0 to 7, each once
Outputs:
- new_weight: float32 [8192, 1024], P(('rep', 'dp'))
- new_moment: float32 [8192, 1024], P(('rep', 'dp'))
- new_second: float32 [8192, 1024], P(('rep', 'dp'))
- new_cold: bfloat16 [8, 8192, 1024], P('dp', 'rep')
- column_sq: float32 [1024], replicated
The draws below stay inside these ranges and needn't reach their ends.
Inputs may be any that keep to these rules, and one draw needn't show every extreme that they name: `ranks`: each block number appears once. `out_grads`: column scales differ from column to column.
All inputs are finite; a program needn't handle non-finite values.
Results may differ from the reference program's by a relative error of at most 0.001.
Values sent between devices are 32-bit elements; how exact they have to be, the bound alone decides.
No kernel may reach another device: no remote copies, remote signals or barrier semaphores. Data moves between devices by JAX's collectives and lax.ppermute only.
A program may use at most 128 MiB of HBM per device.

```python
import math
import jax
import jax.numpy as jnp
from jax import lax

D = 8192
C = 1024
TOK_DEV = 640
BLOCK = 128
NB = 8
HOT = 4
TOKENS = 5120
N_DP = 8


def draw_out_grads(key, part):
    first, second_key = jax.random.split(key, 2)
    base = jax.random.normal(first, (TOKENS, C), jnp.float32)
    col_scale = jnp.exp(jax.random.uniform(second_key, (1, C), jnp.float32, -1.4, 1.4))
    values = base * col_scale
    return jnp.clip(values, -12.0, 12.0).astype(jnp.bfloat16)


def level_of(key, shape, pieces, smallest, high):
    level, own = 1.0, jax.random.fold_in(key, 6)
    for position, shards_of in pieces:
        heights = jnp.exp(jax.random.uniform(jax.random.fold_in(own, position), (shards_of,), jnp.float32, smallest / len(pieces), high / len(pieces)))
        level = level * jnp.repeat(heights, shape[position] // shards_of).reshape([-1 if axis == position else 1 for axis in range(len(shape))])
    return level


def centred(key, dims, width, bound, cuts=(), dtype=jnp.bfloat16):
    gain = level_of(key, dims, cuts, -0.22, 0.18) if cuts else 1.0
    result = jax.random.normal(key, dims, jnp.float32) * width * gain
    return jnp.minimum(jnp.maximum(result, -bound), bound).astype(dtype)


def setup_inputs(seed: int = 0) -> dict:
    keys = jax.random.split(jax.random.key(seed), 8)
    return {
        "features": centred(keys[0], (TOKENS, D), 1.0, 6.0, ((0, 8), (1, 4))),
        "out_grads": draw_out_grads(jax.random.fold_in(keys[7], 71), 0),
        "cold_sums": centred(keys[2], (N_DP, D, C), 16.0, 96.0, ((0, 8), (1, 4))),
        "weight": centred(keys[3], (D, C), 0.5, 3.0, ((0, 32),), jnp.float32),
        "moment": centred(keys[4], (D, C), 1.0, 6.0, ((0, 32),), jnp.float32),
        "second": jnp.clip(jnp.exp(math.log(4.0) - 5.9914646 * jax.random.uniform(keys[5], (D, C), jnp.float32) ** level_of(keys[5], (D, C), ((0, 32),), -0.2, 0.2)), 0.01, 4.0),
        "ranks": jax.random.permutation(keys[6], NB).astype(jnp.int32),
    }


def reference(features, out_grads, cold_sums, weight, moment, second, ranks):
    hot_block = ranks < HOT
    hot_col = jnp.repeat(hot_block, BLOCK)
    feats = features.reshape(N_DP, TOK_DEV, D)
    grads = out_grads.reshape(N_DP, TOK_DEV, C)

    def one_group(carry, inputs):
        summed, squares = carry
        feat, cot, cold = inputs
        local = cold.astype(jnp.float32) + jnp.dot(feat.T, cot, preferred_element_type=jnp.float32)
        kept = jnp.where(hot_col[None, :], jnp.float32(0.0), local).astype(jnp.bfloat16)
        return ((summed + local, squares + lax.optimization_barrier(jnp.sum(local * local, axis=0))), kept)
    start = (jnp.zeros((D, C), jnp.float32), jnp.zeros((C,), jnp.float32))
    (summed, column_sq), new_cold = lax.scan(one_group, start, (feats, grads, cold_sums))
    rms = jnp.sqrt(column_sq / jnp.float32(D * N_DP * TOK_DEV))
    clip = 1.0 / jnp.maximum(jnp.float32(1.0), rms)
    grad_mean = summed * clip[None, :] / jnp.float32(N_DP)
    moved = 0.9 * moment + 0.1 * grad_mean
    squared = 0.95 * second + 0.05 * grad_mean * grad_mean
    step_size = 0.05 * (moved / (1.0 - 0.9 ** 10)) / (jnp.sqrt(squared / (1.0 - 0.95 ** 10)) + 1e-08)
    new_moment = jnp.where(hot_col[None, :], moved, moment)
    new_second = jnp.where(hot_col[None, :], squared, second)
    new_weight = jnp.where(hot_col[None, :], weight - step_size, weight)
    return (new_weight, new_moment, new_second, new_cold, column_sq)
```

```python
import jax
import jax.numpy as jnp
from jax import lax
from jax.sharding import PartitionSpec as P


def cycle(count):
    return list(range(1, count, 2)) + list(reversed(range(0, count, 2)))


def body(features, out_grads, cold_sums, weight, moment, second, ranks):
    blocks = ranks.shape[0]
    hot_count = blocks // 2
    width = out_grads.shape[1]
    local_rows = features.shape[1]
    grad = lax.dot_general(
        features, out_grads, (((0,), (0,)), ((), ())), preferred_element_type=jnp.float32
    )
    local = cold_sums[0].astype(jnp.float32) + grad
    hot_block = ranks < hot_count
    hot_col = jnp.repeat(hot_block, 128)
    new_cold = jnp.where(hot_col[None, :], jnp.float32(0.0), local).astype(jnp.bfloat16)[None]
    partial_sq = jnp.sum(local * local, axis=0)
    column_sq = lax.psum(partial_sq, ("dp", "rep"))
    picker = (ranks[None, :] == jnp.arange(hot_count, dtype=jnp.int32)[:, None]).astype(jnp.float32)
    packed = jnp.einsum(
        "rbk,sb->rsk",
        local.reshape(local_rows, blocks, 128),
        picker,
        precision=lax.Precision.HIGHEST,
    )
    members = cycle(lax.axis_size("dp"))
    part = packed.reshape(len(members), local_rows // len(members), hot_count * 128)
    ordered = jnp.concatenate([part[m] for m in members], axis=0)
    owned = lax.psum_scatter(
        ordered, "dp", scatter_dimension=0, tiled=True, axis_index_groups=[members]
    )
    owned_rows = owned.shape[0]
    spread = jnp.einsum(
        "rsk,sb->rbk",
        owned.reshape(owned_rows, hot_count, 128),
        picker,
        precision=lax.Precision.HIGHEST,
    )
    summed = spread.reshape(owned_rows, width)
    dp_count = lax.axis_size("dp")
    total_rows = local_rows * lax.axis_size("rep")
    rms = jnp.sqrt(column_sq / jnp.float32(total_rows * dp_count * features.shape[0]))
    clip = 1.0 / jnp.maximum(jnp.float32(1.0), rms)
    grad_mean = summed * clip[None, :] / jnp.float32(dp_count)
    moved = 0.9 * moment + 0.1 * grad_mean
    squared = 0.95 * second + 0.05 * grad_mean * grad_mean
    step_size = 0.05 * (moved / (1.0 - 0.9**10)) / (jnp.sqrt(squared / (1.0 - 0.95**10)) + 1e-08)
    new_moment = jnp.where(hot_col[None, :], moved, moment)
    new_second = jnp.where(hot_col[None, :], squared, second)
    new_weight = jnp.where(hot_col[None, :], weight - step_size, weight)
    return (new_weight, new_moment, new_second, new_cold, column_sq)


def solution(mesh):
    placed = (
        P("dp", "rep"),
        P("dp", None),
        P("dp", "rep", None),
        P(("rep", "dp"), None),
        P(("rep", "dp"), None),
        P(("rep", "dp"), None),
        P(),
    )
    return jax.shard_map(
        body,
        mesh=mesh,
        in_specs=placed,
        out_specs=(
            P(("rep", "dp"), None),
            P(("rep", "dp"), None),
            P(("rep", "dp"), None),
            P("dp", "rep", None),
            P(),
        ),
        check_vma=False,
    )
```
